32 devices in a mesh: member: 2 (over x), row: 16 (over z, y, core).
Axes of the slice: x: 2, y: 2, z: 4, core: 2. Of those that a mesh axis runs over, the one named last changes fastest.
Arguments:
- field: float32 [8, 6, 2048, 2048], P('member', None, 'row'), parts along dimension 0, as said below
- host: float32 [128, 2, 8, 6, 128], P('row', None, 'member'), parts along dimension 2, may hold values from -0.12 to 0.12
- weights: float32 [8, 4], replicated, may hold values from 0.1 to 1
- cut_x: int32 [6], replicated, may hold values from 16 to 63
- cut_y: int32 [6], replicated, may hold values from 16 to 63
- table_index: int32 [6], replicated, may hold values from 0 to 7
Outputs:
- nudged: float32 [8, 6, 2048, 2048], P('member', None, 'row'), parts along dimension 0
The draws below stay inside these ranges and needn't reach their ends.
There are 2 independent parts, one for each index of `member`. The reference program is written for one: setup_inputs(seed, part) draws one part's arguments, and reference() takes and returns one part's arrays. A program takes and returns all parts, laid end to end along the dimension named above; an argument that names none is the same for every part. Nothing has to cross between parts.
Inputs may be any that keep to these rules, and one draw needn't show every extreme that they name: `field`: real-valued fields with strong large-scale structure.
All inputs are finite; a program needn't handle non-finite values.
Results may differ from the reference program's by a relative error of at most 0.00005.
Values sent between devices are 32-bit elements; how exact they have to be, the bound alone decides.
A program may use at most 128 MiB of HBM per device.

```python
import math
import jax
import jax.numpy as jnp
from jax import lax

NX = 2048
NY = 2048
VARS = 4
LEVELS = 6
KHALF = 64
TABLE = 8
KBOX = 128


def draw_field(key, part):
    first_key, second_key = jax.random.split(jax.random.fold_in(key, 17), 2)
    signed = jnp.arange(KBOX, dtype=jnp.int32) - KHALF
    phase_x = jnp.mod(jnp.arange(NX, dtype=jnp.int32)[:, None] * signed[None, :], NX).astype(jnp.float32) * (2.0 * math.pi / NX)
    phase_y = jnp.mod(jnp.arange(NY, dtype=jnp.int32)[:, None] * signed[None, :], NY).astype(jnp.float32) * (2.0 * math.pi / NY)
    coeffs = 0.011 * jax.random.normal(second_key, (2, VARS, LEVELS, KBOX, KBOX), jnp.float32)
    noise = 0.5 * jax.random.normal(first_key, (VARS, LEVELS, NX, NY), jnp.float32)
    cos_x = jnp.cos(phase_x)
    sin_x = jnp.sin(phase_x)
    real_part = jnp.einsum('xa,vlab->vlxb', cos_x, coeffs[0]) - jnp.einsum('xa,vlab->vlxb', sin_x, coeffs[1])
    imag_part = jnp.einsum('xa,vlab->vlxb', sin_x, coeffs[0]) + jnp.einsum('xa,vlab->vlxb', cos_x, coeffs[1])
    smooth = jnp.einsum('vlxb,yb->vlxy', real_part, jnp.cos(phase_y)) - jnp.einsum('vlxb,yb->vlxy', imag_part, jnp.sin(phase_y))
    return (smooth + noise).astype(jnp.float32)


def set_ends(drawn, own_key, low, high):
    longest = drawn.shape.index(max(drawn.shape))
    spots = []
    for shift in (0, 1):
        where = [jax.random.randint(jax.random.fold_in(own_key, axis), (), 0, length) for axis, length in enumerate(drawn.shape)]
        where[longest] = (where[longest] + shift) % drawn.shape[longest]
        spots.append(tuple(where))
    return drawn.at[spots[0]].set(low).at[spots[1]].set(high)


def shard_levels(stream_key, shape, pieces, low, high):
    level = 1.0
    for position, blocks in pieces:
        draws = jax.random.uniform(jax.random.fold_in(jax.random.fold_in(stream_key, 6), position), (blocks,), jnp.float32, low / len(pieces), high / len(pieces))
        level = level * jnp.repeat(jnp.exp(draws), shape[position] // blocks).reshape((-1,) + (1,) * (len(shape) - 1 - position))
    return level


def centred(stream_key, extent, spread, limit, cuts=(), kind=jnp.bfloat16):
    values = jax.random.normal(stream_key, extent, jnp.float32) * spread
    if len(cuts) > 0:
        values = shard_levels(stream_key, extent, cuts, -0.22, 0.18) * values
    return jnp.clip(values, min=-limit, max=limit).astype(kind)


def setup_inputs(seed: int = 0, part: int = 0) -> dict:
    keys = jax.random.split(jax.random.key(seed), 7)
    part_splits = jax.random.split(jax.random.fold_in(keys[6], part), 7)
    field = draw_field(jax.random.fold_in(jax.random.fold_in(keys[6], part), 71), part)
    host = centred(part_splits[1], (KBOX, 2, VARS, LEVELS, KBOX), 0.02, 0.12, ((0, 16),), jnp.float32)
    weights = jnp.clip(jnp.exp(jax.random.uniform(keys[2], (TABLE, VARS), jnp.float32, math.log(0.1), math.log(1.0))), 0.1, 1.0)
    cut_x = set_ends(jax.random.randint(keys[3], (LEVELS,), KHALF // 4, KHALF), jax.random.fold_in(keys[3], 1), KHALF // 4, KHALF - 1).astype(jnp.int32)
    cut_y = set_ends(jax.random.randint(keys[4], (LEVELS,), KHALF // 4, KHALF), jax.random.fold_in(keys[4], 1), KHALF // 4, KHALF - 1).astype(jnp.int32)
    table_index = set_ends(jax.random.randint(keys[5], (LEVELS,), 0, TABLE), jax.random.fold_in(keys[5], 1), 0, TABLE - 1).astype(jnp.int32)
    return dict(field=field, host=host, weights=weights, cut_x=cut_x, cut_y=cut_y, table_index=table_index)


def box_wave(index):
    half = index // 2
    return jnp.where(index % 2 == 0, half, jnp.where(index == 1, -KHALF, -half)).astype(jnp.int32)


def reference(field, host, weights, cut_x, cut_y, table_index):
    signed = jnp.arange(KBOX, dtype=jnp.int32) - KHALF
    y_waves = box_wave(jnp.arange(KBOX, dtype=jnp.int32))
    onehot = (table_index[:, None] == jnp.arange(TABLE, dtype=jnp.int32)[None, :]).astype(jnp.float32)
    blend = jnp.dot(onehot, weights, precision=lax.Precision.HIGHEST)
    mask_x = (jnp.abs(signed)[None, :] <= cut_x[:, None]).astype(jnp.float32)
    mask_y = (jnp.abs(y_waves)[None, :] <= cut_y[:, None]).astype(jnp.float32)
    index_x = jnp.mod(signed, NX).astype(jnp.int32)
    index_y = jnp.mod(y_waves, NY).astype(jnp.int32)
    flat = field.reshape(VARS * LEVELS, NX, NY)

    def forward(grid):
        spectrum = jnp.fft.fft2(grid) / (NX * NY)
        boxed = spectrum[index_x[:, None], index_y[None, :]]
        return jnp.stack([jnp.real(boxed), jnp.imag(boxed)], 0).astype(field.dtype)

    boxes = lax.map(forward, flat).reshape(VARS, LEVELS, 2, KBOX, KBOX)
    spectrum = jnp.transpose(boxes, (4, 2, 0, 1, 3))
    scale = blend.T[None, None, :, :, None] * mask_y.T[:, None, None, :, None] * mask_x[None, None, None, :, :]
    delta = scale * (host - spectrum)
    ordered = jnp.transpose(delta, (2, 3, 1, 4, 0)).reshape(VARS * LEVELS, 2, KBOX, KBOX)

    def inverse(pair):
        grid, parts = pair
        boxed = parts[0] + 1j * parts[1]
        whole = jnp.zeros((NX, NY), dtype=boxed.dtype)
        whole = whole.at[index_x[:, None], index_y[None, :]].set(boxed)
        correction = jnp.real(jnp.fft.ifft2(whole)) * (NX * NY)
        return grid + correction.astype(grid.dtype)

    result = lax.map(inverse, (flat, ordered))
    return result.reshape(VARS, LEVELS, NX, NY)
```

```python
import functools
import math

import jax
import jax.numpy as jnp
import numpy as np
from jax import lax
from jax.experimental import pallas as pl
from jax.experimental.pallas import tpu as pltpu
from jax.sharding import PartitionSpec as P

TABLE = 8
MESH = pl.DeviceIdType.MESH
VMEM_BYTES = 36_000_000
GROUP = 3
LAGS = (1, 2, 3)
PREPARE = 1
HIGHEST = lax.Precision.HIGHEST


def box_wave(index, khalf):
    half = index // 2
    return jnp.where(index % 2 == 0, half, jnp.where(index == 1, -khalf, -half))


def wave_tables(positions, length, waves):
    phase = jnp.mod(positions[:, None] * waves[None, :], length).astype(jnp.float32) * (
        2.0 * math.pi / length
    )
    return (jnp.cos(phase), jnp.sin(phase))


def general(field, host, weights, cut_x, cut_y, table_index):
    variables, levels, row_count, ny = field.shape
    owned, kbox = host.shape[0], host.shape[-1]
    fields = variables * levels
    devices = lax.axis_size("row")
    nx = row_count * devices
    place = lax.axis_index("row")
    local_rows = place * row_count + lax.iota(jnp.int32, row_count)
    x_waves = lax.iota(jnp.int32, kbox) - kbox // 2
    y_waves = box_wave(lax.iota(jnp.int32, kbox), kbox // 2)
    own_waves = box_wave(place * owned + lax.iota(jnp.int32, owned), kbox // 2)
    onehot = (table_index[:, None] == lax.iota(jnp.int32, TABLE)[None, :]).astype(jnp.float32)
    blend = jnp.dot(onehot, weights, precision=HIGHEST)
    mask_x = (jnp.abs(x_waves)[None, :] <= cut_x[:, None]).astype(jnp.float32)
    mask_y = (jnp.abs(own_waves)[None, :] <= cut_y[:, None]).astype(jnp.float32)
    scale = blend.T[:, :, None, None] * mask_y[None, :, :, None] * mask_x[None, :, None, :]
    cos_y, sin_y = wave_tables(lax.iota(jnp.int32, ny), ny, y_waves)
    cos_x, sin_x = wave_tables(local_rows, nx, x_waves)
    table_y = jnp.concatenate([cos_y, -sin_y], 1)
    table_x = jnp.stack([jnp.concatenate([cos_x, -sin_x], 1), jnp.concatenate([sin_x, cos_x], 1)])

    def one(pair):
        grid, wanted, factor = pair
        spread = jnp.dot(grid, table_y, precision=HIGHEST).reshape(row_count, 2, kbox)
        parts = jnp.einsum("xck,cxq->kq", spread, table_x, precision=HIGHEST)
        parts = parts.reshape(devices, owned, 2, kbox)
        moved = lax.all_to_all(parts, "row", split_axis=0, concat_axis=0, tiled=True)
        spectrum = jnp.sum(moved, 0) / (nx * ny)
        delta = factor[:, None, :] * (wanted - spectrum)
        box = lax.all_gather(delta, "row", axis=0, tiled=True).reshape(kbox, 2 * kbox)
        back = jnp.einsum("kq,cxq->xck", box, table_x, precision=HIGHEST)
        return grid + jnp.dot(back.reshape(row_count, 2 * kbox), table_y.T, precision=HIGHEST)

    wanted = host.transpose(2, 3, 0, 1, 4).reshape(fields, owned, 2, kbox)
    result = lax.map(
        one, (field.reshape(fields, row_count, ny), wanted, scale.reshape(fields, owned, kbox))
    )
    return result.reshape(field.shape)


def halves(values):
    high = values.astype(jnp.bfloat16)
    return high, (values - high.astype(jnp.float32)).astype(jnp.bfloat16)


def np_halves(values):
    values = values.astype(np.float32)
    high = values.astype(jnp.bfloat16)
    return high, (values - high.astype(np.float32)).astype(jnp.bfloat16)


def real_modes(positions, length, waves, is_sine):
    if isinstance(positions, int):
        positions = np.arange(positions)
    phase = (positions[:, None] * waves[None, :]) % length * (2.0 * np.pi / length)
    return np.where(is_sine[None, :], np.sin(phase), np.cos(phase))


def inverse_kernel(field_ref, modes_ref, back_ref, x_ref, out_ref):
    count, row_count, ny = field_ref.shape
    kbox = x_ref.shape[1] // 3
    owned = modes_ref.shape[2] // count
    parts = []
    for k in range(count):
        high, low = halves(modes_ref[0, :, k * owned : (k + 1) * owned].reshape(kbox, kbox))
        parts.append(
            lax.dot_general(
                x_ref[...],
                jnp.concatenate([high, low, high], 1),
                (((1,), (1,)), ((), ())),
                preferred_element_type=jnp.float32,
            )
        )
    high, low = halves(jnp.concatenate(parts, 0))
    added = jnp.dot(
        jnp.concatenate([high, low, high], 1), back_ref[...], preferred_element_type=jnp.float32
    )
    out_ref[...] = field_ref[...] + added.reshape(field_ref.shape)


def radices(devices):
    bits = devices.bit_length() - 1
    sizes = [2] * min(bits, 1)
    left = bits - len(sizes)
    return sizes + [2] * (left % 2) + [4] * (left // 2)


def stage_lags(sizes):
    steps = [LAGS[0]] + [LAGS[1] if size == 2 else LAGS[2] for size in sizes[1:]]
    steps = steps + steps[::-1]
    return [sum(steps[: stage + 1]) for stage in range(len(steps))]


def box_kernel(
    sizes, lags, norm, weights_hbm, cut_x_hbm, cut_y_hbm, index_hbm, field_hbm, table_hbm, base_hbm,
    turn_hbm, host_hbm, mix_hbm, back_hbm, full_ref, edge_ref, kept_field_ref, back_ref, x_ref,
    part_ref, want_ref, scale_ref, three_ref, table_ref, base_ref, turn_ref, host_ref, mix_ref,
    weights_ref, cut_x_ref, cut_y_ref, index_ref, *scratch
):
    phases = len(sizes)
    got, kept = scratch[:phases], scratch[phases : 2 * phases - 1]
    send_sem, recv_sem, load_sem, fetch_sem = scratch[2 * phases - 1 :]
    fields, row_count, ny = kept_field_ref.shape
    chunks, span, kbox = scale_ref.shape
    group = fields // chunks
    owned, khalf, levels = span // group, kbox // 2, cut_x_ref.shape[0]
    variables = fields // levels
    half = owned // 2
    me = lax.axis_index("row")
    member = lax.axis_index("member")
    strides = [1]
    for size in sizes:
        strides.append(strides[-1] * size)
    mine = [(me // strides[s]) % sizes[s] for s in range(phases)]
    barrier = pltpu.get_barrier_semaphore()

    def digit(step, away):
        return (mine[step] + away) % sizes[step]

    def peer(step, away):
        return (member, me + (digit(step, away) - mine[step]) * strides[step])

    def others(step):
        return range(1, sizes[step])

    def load(chunk):
        block = pl.ds(chunk * group, group)
        return pltpu.make_async_copy(
            field_hbm.at[block], kept_field_ref.at[block], load_sem.at[chunk]
        )

    early = [(table_hbm, table_ref), (base_hbm, base_ref), (turn_hbm.at[me], turn_ref)]
    late = [
        (host_hbm, host_ref), (mix_hbm, mix_ref), (weights_hbm, weights_ref),
        (cut_x_hbm, cut_x_ref), (cut_y_hbm, cut_y_ref), (index_hbm, index_ref),
    ]
    last = [(back_hbm.at[:kbox], back_ref.at[:kbox]), (back_hbm, back_ref.at[kbox:])]
    fetches = [
        pltpu.make_async_copy(source, target, fetch_sem.at[place])
        for place, (source, target) in enumerate(early + late + last)
    ]
    early, late, last = fetches[:3], fetches[3:9], fetches[9:]

    load(0).start()
    for fetch in early:
        fetch.start()
    for chunk in range(1, min(2, chunks)):
        load(chunk).start()
    for fetch in late:
        fetch.start()
    for chunk in range(2, chunks):
        load(chunk).start()
    for fetch in last:
        fetch.start()
    for step in range(phases):
        for away in others(step):
            pl.semaphore_signal(barrier, inc=1, device_id=peer(step, away), device_id_type=MESH)

    def lead(step, value):
        return (slice(None),) * (phases - 1 - step) + (value,)

    def remote(source, target, stage, chunk, step, away):
        return pltpu.make_async_remote_copy(
            src_ref=source,
            dst_ref=target,
            send_sem=send_sem.at[chunk, stage, away - 1],
            recv_sem=recv_sem.at[chunk, stage, away - 1],
            device_id=peer(step, away),
            device_id_type=MESH,
        )

    def held(step):
        return part_ref if step == 0 else kept[step - 1]

    def reduce_copy(step, chunk, away):
        source = held(step).at[(chunk,) + lead(step, digit(step, away))]
        return remote(source, got[step].at[chunk, away - 1], step, chunk, step, away)

    def gather_copy(step, chunk, away):
        fixed = tuple(mine[s] for s in range(step, -1, -1))
        block = full_ref.at[(chunk,) + (slice(None),) * (phases - 1 - step) + fixed]
        return remote(block, block, 2 * phases - 1 - step, chunk, step, away)

    def mixed(values):
        total = 0.0
        for _ in range(3):
            piece = values.astype(jnp.bfloat16)
            values = values - piece.astype(jnp.float32)
            total = total + lax.dot_general(
                piece,
                mix_ref[...],
                (((1,), (1,)), ((), ())),
                preferred_element_type=jnp.float32,
            )
        return total

    def prepare():
        for fetch in late:
            fetch.wait()
        edge = cut_x_ref[0]
        for level in range(levels):
            edge = jnp.maximum(edge, jnp.maximum(cut_x_ref[level], cut_y_ref[level]))
        edge_ref[0] = edge
        cosine, sine = [], []
        for b in range(half):
            plus, minus = host_ref[2 * b], host_ref[2 * b + 1]
            if b == 0:
                minus = jnp.where(me == 0, 0.0, minus)
            cosine.append(plus[0] + minus[0])
            sine.append(-(plus[1] + minus[1]))
        for b in range(half):
            plus, minus = host_ref[2 * b], host_ref[2 * b + 1]
            if b == 0:
                minus = jnp.where(me == 0, 0.0, minus)
            cosine.append(minus[1] - plus[1])
            sine.append(minus[0] - plus[0])
        rows = owned * fields
        cosine = jnp.stack(cosine).reshape(rows, kbox)
        sine = jnp.stack(sine).reshape(rows, kbox)
        modes = mixed(jnp.concatenate([cosine, sine], 1))
        slot = lax.broadcasted_iota(jnp.int32, (owned, kbox), 0)
        wave = me * half + slot % half
        across = lax.broadcasted_iota(jnp.int32, (owned, kbox), 1) % khalf
        times = jnp.where(wave == 0, 1.0, 2.0) * jnp.where(across == 0, norm, 2.0 * norm)
        for field in range(fields):
            variable, level = divmod(field, levels)
            chunk, place = divmod(field, group)
            inside = (across <= cut_x_ref[level]) & (wave <= cut_y_ref[level])
            scale = jnp.where(inside, weights_ref[variable, index_ref[level]], 0.0)
            wanted = [
                modes[(s * levels + level) * variables + variable][None] for s in range(owned)
            ]
            block = pl.ds(place * owned, owned)
            want_ref[chunk, block] = scale * jnp.concatenate(wanted, 0)
            scale_ref[chunk, block] = scale * times

    def advance(stage, chunk):
        if stage < phases:
            total = held(stage)[(chunk,) + lead(stage, mine[stage])]
            for away in others(stage):
                reduce_copy(stage, chunk, away).wait()
                total = total + got[stage][chunk, away - 1]
            if stage + 1 < phases:
                kept[stage][chunk] = total
                for away in others(stage + 1):
                    reduce_copy(stage + 1, chunk, away).start()
            else:
                own = tuple(mine[s] for s in range(phases - 1, -1, -1))
                full_ref[(chunk,) + own] = want_ref[chunk] - scale_ref[chunk] * total
                for away in others(phases - 1):
                    gather_copy(phases - 1, chunk, away).start()
        else:
            step = 2 * phases - 1 - stage
            for away in others(step):
                gather_copy(step, chunk, away).wait()
            if step > 0:
                for away in others(step - 1):
                    gather_copy(step - 1, chunk, away).start()

    def transform(chunk):
        load(chunk).wait()
        block = kept_field_ref[pl.ds(chunk * group, group)].reshape(group * row_count, ny)
        high, low = halves(block)
        both = jnp.dot(high, table_ref[...], preferred_element_type=jnp.float32)
        rest = jnp.dot(low, table_ref[:, :kbox], preferred_element_type=jnp.float32)
        part = both[:, :kbox] + both[:, kbox:] + rest
        cube = tuple(reversed(sizes))
        for k in range(group):
            high, low = halves(part[k * row_count : (k + 1) * row_count])
            moded = lax.dot_general(
                jnp.concatenate([high, low, high], 0),
                three_ref[...],
                (((0,), (0,)), ((), ())),
                preferred_element_type=jnp.float32,
            )
            where = (chunk,) + (slice(None),) * phases + (slice(k * owned, (k + 1) * owned),)
            part_ref[where] = moded.reshape(cube + (owned, kbox))

    for fetch in early:
        fetch.wait()
    turns = turn_ref[...]
    local = base_ref[:row_count] * turns[:1] + base_ref[row_count:] * turns[1:]
    x_high, x_low = halves(local)
    three_ref[...] = jnp.concatenate([x_high, x_high, x_low], 0)
    x_ref[...] = jnp.concatenate([x_high, x_high, x_low], 1)

    def tick(now, _):
        @pl.when(now < chunks)
        def _():
            transform(now)

        @pl.when(now == 0)
        def _():
            pl.semaphore_wait(barrier, sum(size - 1 for size in sizes))

        @pl.when(now < chunks)
        def _():
            for away in others(0):
                reduce_copy(0, now, away).start()

        @pl.when(now == PREPARE)
        def _():
            prepare()

        for stage in range(2 * phases):
            chunk = now - lags[stage]

            @pl.when((chunk >= 0) & (chunk < chunks))
            def _(stage=stage, chunk=chunk):
                advance(stage, chunk)

        return 0

    lax.fori_loop(0, chunks + lags[-1], tick, 0)
    for fetch in last:
        fetch.wait()


def box_modes(devices, chunks, scalars, field, table, base, turn, host, mix, back):
    fields, row_count, ny = field.shape
    owned, kbox = host.shape[0], host.shape[-1]
    span = fields // chunks * owned
    sizes = radices(devices)
    phases = len(sizes)
    cube = tuple(reversed(sizes))
    lags = stage_lags(sizes)

    def buffer(*shape):
        return pltpu.VMEM(shape + (span, kbox), jnp.float32)

    def like(array):
        return pltpu.VMEM(array.shape, array.dtype)

    got = [buffer(chunks, sizes[s] - 1, *cube[: phases - 1 - s]) for s in range(phases)]
    kept = [buffer(chunks, *cube[: phases - 1 - s]) for s in range(phases - 1)]
    smem = pl.BlockSpec(memory_space=pltpu.SMEM)
    vmem = pl.BlockSpec(memory_space=pltpu.VMEM)
    anywhere = pl.BlockSpec(memory_space=pl.ANY)
    widest = max(sizes) - 1
    return pl.pallas_call(
        functools.partial(box_kernel, sizes, lags, 1.0 / (row_count * devices * ny)),
        out_shape=(
            buffer(chunks, *cube),
            jax.ShapeDtypeStruct((1,), jnp.int32),
            pltpu.VMEM(field.shape, jnp.float32),
            pltpu.VMEM((3 * kbox, ny), jnp.bfloat16),
            pltpu.VMEM((row_count, 3 * kbox), jnp.bfloat16),
        ),
        in_specs=[anywhere] * 11,
        out_specs=(vmem, smem, vmem, vmem, vmem),
        scratch_shapes=[buffer(chunks, *cube)]
        + [buffer(chunks)] * 2
        + [pltpu.VMEM((3 * row_count, kbox), jnp.bfloat16)]
        + [like(table), like(base), pltpu.VMEM(turn.shape[1:], turn.dtype), like(host), like(mix)]
        + [pltpu.SMEM(array.shape, array.dtype) for array in scalars]
        + got
        + kept
        + [
            pltpu.SemaphoreType.DMA((chunks, 2 * phases, widest)),
            pltpu.SemaphoreType.DMA((chunks, 2 * phases, widest)),
            pltpu.SemaphoreType.DMA((chunks,)),
            pltpu.SemaphoreType.DMA((11,)),
        ],
        compiler_params=pltpu.CompilerParams(
            collective_id=0, has_side_effects=True, vmem_limit_bytes=VMEM_BYTES
        ),
    )(*scalars, field, table, base, turn, host, mix, back)


def nudge(field, host, weights, cut_x, cut_y, table_index):
    variables, levels, row_count, ny = field.shape
    owned, kbox = host.shape[0], host.shape[-1]
    khalf, half = kbox // 2, owned // 2
    devices = lax.axis_size("row")
    nx = row_count * devices
    fields = variables * levels
    group = max(size for size in range(1, GROUP + 1) if fields % size == 0)
    chunks = fields // group

    column = np.arange(kbox)
    y_wave = column // owned * half + column % half
    y_sine = column % owned >= half
    y_high, y_low = np_halves(real_modes(ny, ny, y_wave, y_sine))
    table_y = jnp.asarray(np.concatenate([y_high, y_low], 1))
    table_back = jnp.asarray(np.concatenate([y_high.T, y_low.T], 0))
    x_wave, x_sine = column % khalf, column >= khalf
    start = np.arange(devices) * row_count
    base = np.concatenate(
        [real_modes(row_count, nx, x_wave, column < 0), real_modes(row_count, nx, x_wave, column >= 0)]
    )
    turn_cos = real_modes(start, nx, x_wave, column < 0)
    turn_sin = real_modes(start, nx, x_wave, column >= 0)
    turn = np.stack(
        [np.where(x_sine, turn_sin, turn_cos), np.where(x_sine, turn_cos, -turn_sin)], 1
    )
    base = jnp.asarray(base.astype(np.float32))
    turn = jnp.asarray(turn.astype(np.float32))
    wave = column - khalf
    inside = np.abs(wave) < khalf
    mc = ((column[:, None] == np.abs(wave)[None, :]) & inside).astype(np.float32)
    ms = ((column[:, None] == np.abs(wave)[None, :] + khalf) & inside) * np.sign(wave)
    ms = ms.astype(np.float32)

    span = group * owned
    modes, edge, kept_field, back, local = box_modes(
        devices,
        chunks,
        (weights.T, cut_x, cut_y, table_index),
        field.reshape(fields, row_count, ny),
        table_y,
        base,
        turn,
        host.transpose(0, 1, 3, 2, 4),
        jnp.asarray(np.concatenate([mc, ms], 1)).astype(jnp.bfloat16),
        table_back,
    )
    modes = modes.reshape(chunks, devices, span, kbox)

    def inverse(kept_field, modes, back, local):
        grid_block = pl.BlockSpec((group, row_count, ny), lambda g: (g, 0, 0))
        result = pl.pallas_call(
            inverse_kernel,
            grid=(chunks,),
            out_shape=jax.ShapeDtypeStruct(kept_field.shape, jnp.float32),
            in_specs=[
                grid_block,
                pl.BlockSpec((1, devices, span, kbox), lambda g: (g, 0, 0, 0)),
                pl.BlockSpec(back.shape, lambda g: (0, 0)),
                pl.BlockSpec(local.shape, lambda g: (0, 0)),
            ],
            out_specs=grid_block,
            compiler_params=pltpu.CompilerParams(vmem_limit_bytes=VMEM_BYTES),
        )(kept_field, modes, back, local)
        return result.reshape(field.shape)

    return lax.cond(
        edge[0] >= khalf,
        lambda *args: general(*args[:6]),
        lambda *args: inverse(*args[6:]),
        field, host, weights, cut_x, cut_y, table_index, kept_field, modes, back, local,
    )


def solution(mesh):
    return jax.shard_map(
        nudge,
        mesh=mesh,
        in_specs=(
            P("member", None, "row", None),
            P("row", None, "member", None, None),
            P(),
            P(),
            P(),
            P(),
        ),
        out_specs=P("member", None, "row", None),
        check_vma=False,
    )
```

```python
import functools
import math

import jax
import jax.numpy as jnp
import numpy as np
from jax import lax
from jax.experimental import pallas as pl
from jax.experimental.pallas import tpu as pltpu
from jax.sharding import PartitionSpec as P

TABLE = 8
MESH = pl.DeviceIdType.MESH
VMEM_BYTES = 36_000_000
GROUP = 3
LAGS = (1, 2, 2)
PREPARE = 1
AHEAD = 3
HIGHEST = lax.Precision.HIGHEST


def box_wave(index, khalf):
    half = index // 2
    return jnp.where(index % 2 == 0, half, jnp.where(index == 1, -khalf, -half))


def wave_tables(positions, length, waves):
    phase = jnp.mod(positions[:, None] * waves[None, :], length).astype(jnp.float32) * (
        2.0 * math.pi / length
    )
    return (jnp.cos(phase), jnp.sin(phase))


def general(field, host, weights, cut_x, cut_y, table_index):
    variables, levels, row_count, ny = field.shape
    owned, kbox = host.shape[0], host.shape[-1]
    fields = variables * levels
    devices = lax.axis_size("row")
    nx = row_count * devices
    place = lax.axis_index("row")
    local_rows = place * row_count + lax.iota(jnp.int32, row_count)
    x_waves = lax.iota(jnp.int32, kbox) - kbox // 2
    y_waves = box_wave(lax.iota(jnp.int32, kbox), kbox // 2)
    own_waves = box_wave(place * owned + lax.iota(jnp.int32, owned), kbox // 2)
    onehot = (table_index[:, None] == lax.iota(jnp.int32, TABLE)[None, :]).astype(jnp.float32)
    blend = jnp.dot(onehot, weights, precision=HIGHEST)
    mask_x = (jnp.abs(x_waves)[None, :] <= cut_x[:, None]).astype(jnp.float32)
    mask_y = (jnp.abs(own_waves)[None, :] <= cut_y[:, None]).astype(jnp.float32)
    scale = blend.T[:, :, None, None] * mask_y[None, :, :, None] * mask_x[None, :, None, :]
    cos_y, sin_y = wave_tables(lax.iota(jnp.int32, ny), ny, y_waves)
    cos_x, sin_x = wave_tables(local_rows, nx, x_waves)
    table_y = jnp.concatenate([cos_y, -sin_y], 1)
    table_x = jnp.stack([jnp.concatenate([cos_x, -sin_x], 1), jnp.concatenate([sin_x, cos_x], 1)])

    def one(pair):
        grid, wanted, factor = pair
        spread = jnp.dot(grid, table_y, precision=HIGHEST).reshape(row_count, 2, kbox)
        parts = jnp.einsum("xck,cxq->kq", spread, table_x, precision=HIGHEST)
        parts = parts.reshape(devices, owned, 2, kbox)
        moved = lax.all_to_all(parts, "row", split_axis=0, concat_axis=0, tiled=True)
        spectrum = jnp.sum(moved, 0) / (nx * ny)
        delta = factor[:, None, :] * (wanted - spectrum)
        box = lax.all_gather(delta, "row", axis=0, tiled=True).reshape(kbox, 2 * kbox)
        back = jnp.einsum("kq,cxq->xck", box, table_x, precision=HIGHEST)
        return grid + jnp.dot(back.reshape(row_count, 2 * kbox), table_y.T, precision=HIGHEST)

    wanted = host.transpose(2, 3, 0, 1, 4).reshape(fields, owned, 2, kbox)
    result = lax.map(
        one, (field.reshape(fields, row_count, ny), wanted, scale.reshape(fields, owned, kbox))
    )
    return result.reshape(field.shape)


def halves(values):
    high = values.astype(jnp.bfloat16)
    return high, (values - high.astype(jnp.float32)).astype(jnp.bfloat16)


def np_halves(values):
    values = values.astype(np.float32)
    high = values.astype(jnp.bfloat16)
    return high, (values - high.astype(np.float32)).astype(jnp.bfloat16)


def real_modes(positions, length, waves, is_sine):
    if isinstance(positions, int):
        positions = np.arange(positions)
    phase = (positions[:, None] * waves[None, :]) % length * (2.0 * np.pi / length)
    return np.where(is_sine[None, :], np.sin(phase), np.cos(phase))


def inverse_kernel(field_ref, modes_ref, back_ref, x_ref, out_hbm, out_ref, sem):
    chunks, count = field_ref.shape[:2]
    owned = modes_ref.shape[2] // count

    def store(chunk):
        return pltpu.make_async_copy(out_ref.at[chunk], out_hbm.at[chunk], sem.at[chunk])

    def step(chunk, _):
        inverse_step(chunk, count, owned, field_ref, modes_ref, back_ref, x_ref, out_ref)
        store(chunk).start()
        return 0

    lax.fori_loop(0, chunks, step, 0)
    for chunk in range(chunks):
        store(chunk).wait()


def inverse_step(chunk, count, owned, field_ref, modes_ref, back_ref, x_ref, out_ref):
    row_count, ny = field_ref.shape[2:]
    kbox = x_ref.shape[1] // 3
    parts = []
    for k in range(count):
        block = modes_ref[chunk, :, k * owned : (k + 1) * owned]
        swapped = jnp.concatenate([block[:, owned // 2 :], block[:, : owned // 2]], 1)
        both = jnp.concatenate([block.reshape(kbox, kbox), swapped.reshape(kbox, kbox)], 0)
        high, low = halves(both)
        parts.append(
            lax.dot_general(
                x_ref[...],
                jnp.concatenate([high, low, high], 1),
                (((1,), (1,)), ((), ())),
                preferred_element_type=jnp.float32,
            )
        )
    spread = jnp.concatenate(parts, 0)
    high = spread[:, :kbox].astype(jnp.bfloat16)
    low = (spread[:, kbox:] - spread[:, kbox:].astype(jnp.bfloat16).astype(jnp.float32)).astype(
        jnp.bfloat16
    )
    lane = lax.broadcasted_iota(jnp.int32, high.shape, 1)
    first = lane % owned < owned // 2
    even = jnp.where(first, high, low)
    odd = jnp.where(first, low, high)
    shape = (count, row_count, ny // 2)
    plus = jnp.dot(
        jnp.concatenate([even, even], 1), back_ref[0], preferred_element_type=jnp.float32
    ).reshape(shape)
    minus = jnp.dot(
        jnp.concatenate([odd, odd], 1), back_ref[1], preferred_element_type=jnp.float32
    ).reshape(shape)
    out_ref[chunk, :, :, : ny // 2] = field_ref[chunk, :, :, : ny // 2] + (plus + minus)
    out_ref[chunk, :, :, ny // 2 :] = field_ref[chunk, :, :, ny // 2 :] + (plus - minus)


def radices(devices):
    bits = devices.bit_length() - 1
    sizes = [2] * min(bits, 1)
    left = bits - len(sizes)
    return sizes + [2] * (left % 2) + [4] * (left // 2)


def stage_lags(sizes):
    steps = [LAGS[0]] + [LAGS[1] if size == 2 else LAGS[2] for size in sizes[1:]]
    steps = steps + steps[::-1]
    return [sum(steps[: stage + 1]) for stage in range(len(steps))]


def box_kernel(
    sizes, lags, norm, weights_hbm, cut_x_hbm, cut_y_hbm, index_hbm, field_hbm, table_hbm, base_hbm,
    turn_hbm, host_hbm, mix_hbm, back_hbm, full_ref, edge_ref, kept_field_ref, back_ref, x_ref,
    part_ref, want_ref, scale_ref, three_ref, table_ref, base_ref, turn_ref, host_ref, mix_ref,
    weights_ref, cut_x_ref, cut_y_ref, index_ref, *scratch
):
    phases = len(sizes)
    got, kept = scratch[:phases], scratch[phases : 2 * phases - 1]
    send_sem, recv_sem, load_sem, fetch_sem = scratch[2 * phases - 1 :]
    fields, row_count, ny = kept_field_ref.shape
    chunks, span, kbox = scale_ref.shape
    group = fields // chunks
    owned, khalf, levels = span // group, kbox // 2, cut_x_ref.shape[0]
    variables = fields // levels
    half = owned // 2
    me = lax.axis_index("row")
    member = lax.axis_index("member")
    strides = [1]
    for size in sizes:
        strides.append(strides[-1] * size)
    mine = [(me // strides[s]) % sizes[s] for s in range(phases)]
    barrier = pltpu.get_barrier_semaphore()

    def digit(step, away):
        return (mine[step] + away) % sizes[step]

    def peer(step, away):
        return (member, me + (digit(step, away) - mine[step]) * strides[step])

    def others(step):
        return range(1, sizes[step])

    def load(chunk):
        block = pl.ds(chunk * group, group)
        return pltpu.make_async_copy(
            field_hbm.at[block], kept_field_ref.at[block], load_sem.at[chunk]
        )

    early = [(table_hbm, table_ref), (base_hbm, base_ref), (turn_hbm.at[me], turn_ref)]
    late = [
        (host_hbm, host_ref), (mix_hbm, mix_ref), (weights_hbm, weights_ref),
        (cut_x_hbm, cut_x_ref), (cut_y_hbm, cut_y_ref), (index_hbm, index_ref),
    ]
    last = [(back_hbm, back_ref)]
    fetches = [
        pltpu.make_async_copy(source, target, fetch_sem.at[place])
        for place, (source, target) in enumerate(early + late + last)
    ]
    early, late, last = fetches[:3], fetches[3:9], fetches[9:]

    load(0).start()
    for fetch in early:
        fetch.start()
    for fetch in late:
        fetch.start()
    for chunk in range(1, min(AHEAD, chunks)):
        load(chunk).start()
    for step in range(phases):
        for away in others(step):
            pl.semaphore_signal(barrier, inc=1, device_id=peer(step, away), device_id_type=MESH)

    def lead(step, value):
        return (slice(None),) * (phases - 1 - step) + (value,)

    def remote(source, target, stage, chunk, step, away):
        return pltpu.make_async_remote_copy(
            src_ref=source,
            dst_ref=target,
            send_sem=send_sem.at[chunk, stage, away - 1],
            recv_sem=recv_sem.at[chunk, stage, away - 1],
            device_id=peer(step, away),
            device_id_type=MESH,
        )

    def held(step):
        return part_ref if step == 0 else kept[step - 1]

    def reduce_copy(step, chunk, away):
        source = held(step).at[(chunk,) + lead(step, digit(step, away))]
        return remote(source, got[step].at[chunk, away - 1], step, chunk, step, away)

    def gather_copy(step, chunk, away):
        fixed = tuple(mine[s] for s in range(step, -1, -1))
        block = full_ref.at[(chunk,) + (slice(None),) * (phases - 1 - step) + fixed]
        return remote(block, block, 2 * phases - 1 - step, chunk, step, away)

    def mixed(values):
        total = 0.0
        for _ in range(3):
            piece = values.astype(jnp.bfloat16)
            values = values - piece.astype(jnp.float32)
            total = total + lax.dot_general(
                piece,
                mix_ref[...],
                (((1,), (1,)), ((), ())),
                preferred_element_type=jnp.float32,
            )
        return total

    def prepare():
        for fetch in late:
            fetch.wait()
        edge = cut_x_ref[0]
        for level in range(levels):
            edge = jnp.maximum(edge, jnp.maximum(cut_x_ref[level], cut_y_ref[level]))
        edge_ref[0] = edge
        cosine, sine = [], []
        for place in range(owned):
            pair = 2 * (place % (half // 2)) + place // half
            plus, minus = host_ref[2 * pair], host_ref[2 * pair + 1]
            if pair == 0:
                minus = jnp.where(me == 0, 0.0, minus)
            if place // (half // 2) % 2 == 0:
                cosine.append(plus[0] + minus[0])
                sine.append(-(plus[1] + minus[1]))
            else:
                cosine.append(minus[1] - plus[1])
                sine.append(minus[0] - plus[0])
        rows = owned * fields
        cosine = jnp.stack(cosine).reshape(rows, kbox)
        sine = jnp.stack(sine).reshape(rows, kbox)
        modes = mixed(jnp.concatenate([cosine, sine], 1))
        slot = lax.broadcasted_iota(jnp.int32, (owned, kbox), 0)
        wave = me * half + 2 * (slot % (half // 2)) + slot // half
        across = lax.broadcasted_iota(jnp.int32, (owned, kbox), 1) % khalf
        times = jnp.where(wave == 0, 1.0, 2.0) * jnp.where(across == 0, norm, 2.0 * norm)
        for field in range(fields):
            variable, level = divmod(field, levels)
            chunk, place = divmod(field, group)
            inside = (across <= cut_x_ref[level]) & (wave <= cut_y_ref[level])
            scale = jnp.where(inside, weights_ref[variable, index_ref[level]], 0.0)
            wanted = [
                modes[(s * levels + level) * variables + variable][None] for s in range(owned)
            ]
            block = pl.ds(place * owned, owned)
            want_ref[chunk, block] = scale * jnp.concatenate(wanted, 0)
            scale_ref[chunk, block] = scale * times

    def advance(stage, chunk):
        if stage < phases:
            total = held(stage)[(chunk,) + lead(stage, mine[stage])]
            for away in others(stage):
                reduce_copy(stage, chunk, away).wait()
                total = total + got[stage][chunk, away - 1]
            if stage + 1 < phases:
                kept[stage][chunk] = total
                for away in others(stage + 1):
                    reduce_copy(stage + 1, chunk, away).start()
            else:
                own = tuple(mine[s] for s in range(phases - 1, -1, -1))
                full_ref[(chunk,) + own] = want_ref[chunk] - scale_ref[chunk] * total
                for away in others(phases - 1):
                    gather_copy(phases - 1, chunk, away).start()
        else:
            step = 2 * phases - 1 - stage
            for away in others(step):
                gather_copy(step, chunk, away).wait()
            if step > 0:
                for away in others(step - 1):
                    gather_copy(step - 1, chunk, away).start()

    def transform(chunk):
        load(chunk).wait()

        @pl.when(chunk + AHEAD < chunks)
        def _():
            load(chunk + AHEAD).start()

        block = kept_field_ref[pl.ds(chunk * group, group)].reshape(group * row_count, ny)
        high, low = halves(block)
        both = jnp.dot(high, table_ref[...], preferred_element_type=jnp.float32)
        rest = jnp.dot(low, table_ref[:, :kbox], preferred_element_type=jnp.float32)
        part = both[:, :kbox] + both[:, kbox:] + rest
        cube = tuple(reversed(sizes))
        for k in range(group):
            high, low = halves(part[k * row_count : (k + 1) * row_count])
            moded = lax.dot_general(
                jnp.concatenate([high, low, high], 0),
                three_ref[...],
                (((0,), (0,)), ((), ())),
                preferred_element_type=jnp.float32,
            )
            where = (chunk,) + (slice(None),) * phases + (slice(k * owned, (k + 1) * owned),)
            part_ref[where] = moded.reshape(cube + (owned, kbox))

    for fetch in early:
        fetch.wait()
    turns = turn_ref[...]
    local = base_ref[:row_count] * turns[:1] + base_ref[row_count:] * turns[1:]
    x_high, x_low = halves(local)
    three_ref[...] = jnp.concatenate([x_high, x_high, x_low], 0)
    x_ref[...] = jnp.concatenate([x_high, x_high, x_low], 1)

    def tick(now, _):
        @pl.when(now < chunks)
        def _():
            transform(now)

        @pl.when(now == 0)
        def _():
            pl.semaphore_wait(barrier, sum(size - 1 for size in sizes))

        @pl.when(now < chunks)
        def _():
            for away in others(0):
                reduce_copy(0, now, away).start()

        @pl.when(now == PREPARE)
        def _():
            prepare()

        @pl.when(now == chunks - 1)
        def _():
            for fetch in last:
                fetch.start()

        for stage in range(2 * phases):
            chunk = now - lags[stage]

            @pl.when((chunk >= 0) & (chunk < chunks))
            def _(stage=stage, chunk=chunk):
                advance(stage, chunk)

        return 0

    lax.fori_loop(0, chunks + lags[-1], tick, 0)
    for fetch in last:
        fetch.wait()


def box_modes(devices, chunks, scalars, field, table, base, turn, host, mix, back):
    fields, row_count, ny = field.shape
    owned, kbox = host.shape[0], host.shape[-1]
    span = fields // chunks * owned
    sizes = radices(devices)
    phases = len(sizes)
    cube = tuple(reversed(sizes))
    lags = stage_lags(sizes)

    def buffer(*shape):
        return pltpu.VMEM(shape + (span, kbox), jnp.float32)

    def like(array):
        return pltpu.VMEM(array.shape, array.dtype)

    got = [buffer(chunks, sizes[s] - 1, *cube[: phases - 1 - s]) for s in range(phases)]
    kept = [buffer(chunks, *cube[: phases - 1 - s]) for s in range(phases - 1)]
    smem = pl.BlockSpec(memory_space=pltpu.SMEM)
    vmem = pl.BlockSpec(memory_space=pltpu.VMEM)
    anywhere = pl.BlockSpec(memory_space=pl.ANY)
    widest = max(sizes) - 1
    return pl.pallas_call(
        functools.partial(box_kernel, sizes, lags, 1.0 / (row_count * devices * ny)),
        out_shape=(
            buffer(chunks, *cube),
            jax.ShapeDtypeStruct((1,), jnp.int32),
            pltpu.VMEM(field.shape, jnp.float32),
            like(back),
            pltpu.VMEM((row_count, 3 * kbox), jnp.bfloat16),
        ),
        in_specs=[anywhere] * 11,
        out_specs=(vmem, smem, vmem, vmem, vmem),
        scratch_shapes=[buffer(chunks, *cube)]
        + [buffer(chunks)] * 2
        + [pltpu.VMEM((3 * row_count, kbox), jnp.bfloat16)]
        + [like(table), like(base), pltpu.VMEM(turn.shape[1:], turn.dtype), like(host), like(mix)]
        + [pltpu.SMEM(array.shape, array.dtype) for array in scalars]
        + got
        + kept
        + [
            pltpu.SemaphoreType.DMA((chunks, 2 * phases, widest)),
            pltpu.SemaphoreType.DMA((chunks, 2 * phases, widest)),
            pltpu.SemaphoreType.DMA((chunks,)),
            pltpu.SemaphoreType.DMA((10,)),
        ],
        compiler_params=pltpu.CompilerParams(
            collective_id=0, has_side_effects=True, vmem_limit_bytes=VMEM_BYTES
        ),
    )(*scalars, field, table, base, turn, host, mix, back)


def nudge(field, host, weights, cut_x, cut_y, table_index):
    variables, levels, row_count, ny = field.shape
    owned, kbox = host.shape[0], host.shape[-1]
    khalf, half = kbox // 2, owned // 2
    devices = lax.axis_size("row")
    nx = row_count * devices
    fields = variables * levels
    group = max(size for size in range(1, GROUP + 1) if fields % size == 0)
    chunks = fields // group

    column = np.arange(kbox)
    y_odd, y_sine, y_place = column // half % 2, column // (half // 2) % 2 == 1, column % (half // 2)
    y_wave = column // owned * half + 2 * y_place + y_odd
    y_high, y_low = np_halves(real_modes(ny, ny, y_wave, y_sine))
    table_y = jnp.asarray(np.concatenate([y_high, y_low], 1))
    backs = []
    for odd in (0, 1):
        twin = np.where(y_odd == odd, column, (column + half) % owned + column // owned * owned)
        high, low = np_halves(real_modes(ny // 2, ny, y_wave[twin], y_sine[twin]).T)
        backs.append(np.concatenate([high, low], 0))
    table_back = jnp.asarray(np.stack(backs))
    x_wave, x_sine = column % khalf, column >= khalf
    start = np.arange(devices) * row_count
    base = np.concatenate(
        [real_modes(row_count, nx, x_wave, column < 0), real_modes(row_count, nx, x_wave, column >= 0)]
    )
    turn_cos = real_modes(start, nx, x_wave, column < 0)
    turn_sin = real_modes(start, nx, x_wave, column >= 0)
    turn = np.stack(
        [np.where(x_sine, turn_sin, turn_cos), np.where(x_sine, turn_cos, -turn_sin)], 1
    )
    base = jnp.asarray(base.astype(np.float32))
    turn = jnp.asarray(turn.astype(np.float32))
    wave = column - khalf
    inside = np.abs(wave) < khalf
    mc = ((column[:, None] == np.abs(wave)[None, :]) & inside).astype(np.float32)
    ms = ((column[:, None] == np.abs(wave)[None, :] + khalf) & inside) * np.sign(wave)
    ms = ms.astype(np.float32)

    span = group * owned
    modes, edge, kept_field, back, local = box_modes(
        devices,
        chunks,
        (weights.T, cut_x, cut_y, table_index),
        field.reshape(fields, row_count, ny),
        table_y,
        base,
        turn,
        host.transpose(0, 1, 3, 2, 4),
        jnp.asarray(np.concatenate([mc, ms], 1)).astype(jnp.bfloat16),
        table_back,
    )
    modes = modes.reshape(chunks, devices, span, kbox)

    def inverse(kept_field, modes, back, local):
        split = (chunks, group, row_count, ny)
        vmem = pl.BlockSpec(memory_space=pltpu.VMEM)
        result = pl.pallas_call(
            inverse_kernel,
            out_shape=jax.ShapeDtypeStruct(split, jnp.float32),
            in_specs=[vmem] * 4,
            out_specs=pl.BlockSpec(memory_space=pl.ANY),
            scratch_shapes=[
                pltpu.VMEM(split, jnp.float32), pltpu.SemaphoreType.DMA((chunks,))
            ],
            compiler_params=pltpu.CompilerParams(vmem_limit_bytes=VMEM_BYTES),
        )(kept_field.reshape(split), modes, back, local)
        return result.reshape(field.shape)

    return lax.cond(
        edge[0] >= khalf,
        lambda *args: general(*args[:6]),
        lambda *args: inverse(*args[6:]),
        field, host, weights, cut_x, cut_y, table_index, kept_field, modes, back, local,
    )


def solution(mesh):
    return jax.shard_map(
        nudge,
        mesh=mesh,
        in_specs=(
            P("member", None, "row", None),
            P("row", None, "member", None, None),
            P(),
            P(),
            P(),
            P(),
        ),
        out_specs=P("member", None, "row", None),
        check_vma=False,
    )
```

```python
import functools
import math

import jax
import jax.numpy as jnp
import numpy as np
from jax import lax
from jax.experimental import pallas as pl
from jax.experimental.pallas import tpu as pltpu
from jax.sharding import PartitionSpec as P

TABLE = 8
MESH = pl.DeviceIdType.MESH
VMEM_BYTES = 36_000_000
GROUP = 3
LAGS = (1, 2, 2)
PREPARE = 1
READY = 1
AHEAD = 3
HIGHEST = lax.Precision.HIGHEST


def box_wave(index, khalf):
    half = index // 2
    return jnp.where(index % 2 == 0, half, jnp.where(index == 1, -khalf, -half))


def wave_tables(positions, length, waves):
    phase = jnp.mod(positions[:, None] * waves[None, :], length).astype(jnp.float32) * (
        2.0 * math.pi / length
    )
    return (jnp.cos(phase), jnp.sin(phase))


def general(field, host, weights, cut_x, cut_y, table_index):
    variables, levels, row_count, ny = field.shape
    owned, kbox = host.shape[0], host.shape[-1]
    fields = variables * levels
    devices = lax.axis_size("row")
    nx = row_count * devices
    place = lax.axis_index("row")
    local_rows = place * row_count + lax.iota(jnp.int32, row_count)
    x_waves = lax.iota(jnp.int32, kbox) - kbox // 2
    y_waves = box_wave(lax.iota(jnp.int32, kbox), kbox // 2)
    own_waves = box_wave(place * owned + lax.iota(jnp.int32, owned), kbox // 2)
    onehot = (table_index[:, None] == lax.iota(jnp.int32, TABLE)[None, :]).astype(jnp.float32)
    blend = jnp.dot(onehot, weights, precision=HIGHEST)
    mask_x = (jnp.abs(x_waves)[None, :] <= cut_x[:, None]).astype(jnp.float32)
    mask_y = (jnp.abs(own_waves)[None, :] <= cut_y[:, None]).astype(jnp.float32)
    scale = blend.T[:, :, None, None] * mask_y[None, :, :, None] * mask_x[None, :, None, :]
    cos_y, sin_y = wave_tables(lax.iota(jnp.int32, ny), ny, y_waves)
    cos_x, sin_x = wave_tables(local_rows, nx, x_waves)
    table_y = jnp.concatenate([cos_y, -sin_y], 1)
    table_x = jnp.stack([jnp.concatenate([cos_x, -sin_x], 1), jnp.concatenate([sin_x, cos_x], 1)])

    def one(pair):
        grid, wanted, factor = pair
        spread = jnp.dot(grid, table_y, precision=HIGHEST).reshape(row_count, 2, kbox)
        parts = jnp.einsum("xck,cxq->kq", spread, table_x, precision=HIGHEST)
        parts = parts.reshape(devices, owned, 2, kbox)
        moved = lax.all_to_all(parts, "row", split_axis=0, concat_axis=0, tiled=True)
        spectrum = jnp.sum(moved, 0) / (nx * ny)
        delta = factor[:, None, :] * (wanted - spectrum)
        box = lax.all_gather(delta, "row", axis=0, tiled=True).reshape(kbox, 2 * kbox)
        back = jnp.einsum("kq,cxq->xck", box, table_x, precision=HIGHEST)
        return grid + jnp.dot(back.reshape(row_count, 2 * kbox), table_y.T, precision=HIGHEST)

    wanted = host.transpose(2, 3, 0, 1, 4).reshape(fields, owned, 2, kbox)
    result = lax.map(
        one, (field.reshape(fields, row_count, ny), wanted, scale.reshape(fields, owned, kbox))
    )
    return result.reshape(field.shape)


def halves(values):
    high = values.astype(jnp.bfloat16)
    return high, (values - high.astype(jnp.float32)).astype(jnp.bfloat16)


def np_halves(values):
    values = values.astype(np.float32)
    high = values.astype(jnp.bfloat16)
    return high, (values - high.astype(np.float32)).astype(jnp.bfloat16)


def real_modes(positions, length, waves, is_sine):
    if isinstance(positions, int):
        positions = np.arange(positions)
    phase = (positions[:, None] * waves[None, :]) % length * (2.0 * np.pi / length)
    return np.where(is_sine[None, :], np.sin(phase), np.cos(phase))


def inverse_kernel(field_ref, modes_ref, back_ref, x_ref, out_hbm, out_ref, sem):
    chunks, count = field_ref.shape[:2]

    def store(chunk, source):
        return pltpu.make_async_copy(source.at[chunk], out_hbm.at[chunk], sem.at[chunk])

    def step(chunk, _):
        inverse_step(count, field_ref.at[chunk], modes_ref[chunk], back_ref, x_ref, out_ref.at[chunk])
        store(chunk, out_ref).start()
        return 0

    for chunk in range(READY):
        store(chunk, field_ref).start()
    lax.fori_loop(READY, chunks, step, 0)
    for chunk in range(chunks):
        store(chunk, field_ref if chunk < READY else out_ref).wait()


def inverse_step(count, field_ref, modes, back_ref, x_ref, out_ref):
    row_count, ny = field_ref.shape[1:]
    kbox = x_ref.shape[1] // 3
    owned = modes.shape[1] // count
    parts = []
    for k in range(count):
        block = modes[:, k * owned : (k + 1) * owned]
        swapped = jnp.concatenate([block[:, owned // 2 :], block[:, : owned // 2]], 1)
        both = jnp.concatenate([block.reshape(kbox, kbox), swapped.reshape(kbox, kbox)], 0)
        high, low = halves(both)
        parts.append(
            lax.dot_general(
                x_ref[...],
                jnp.concatenate([high, low, high], 1),
                (((1,), (1,)), ((), ())),
                preferred_element_type=jnp.float32,
            )
        )
    spread = jnp.concatenate(parts, 0)
    high = spread[:, :kbox].astype(jnp.bfloat16)
    low = (spread[:, kbox:] - spread[:, kbox:].astype(jnp.bfloat16).astype(jnp.float32)).astype(
        jnp.bfloat16
    )
    lane = lax.broadcasted_iota(jnp.int32, high.shape, 1)
    first = lane % owned < owned // 2
    even = jnp.where(first, high, low)
    odd = jnp.where(first, low, high)
    shape = (count, row_count, ny // 2)
    plus = jnp.dot(
        jnp.concatenate([even, even], 1), back_ref[0], preferred_element_type=jnp.float32
    ).reshape(shape)
    minus = jnp.dot(
        jnp.concatenate([odd, odd], 1), back_ref[1], preferred_element_type=jnp.float32
    ).reshape(shape)
    out_ref[:, :, : ny // 2] = field_ref[:, :, : ny // 2] + (plus + minus)
    out_ref[:, :, ny // 2 :] = field_ref[:, :, ny // 2 :] + (plus - minus)


def radices(devices):
    bits = devices.bit_length() - 1
    sizes = [2] * min(bits, 1)
    left = bits - len(sizes)
    return sizes + [2] * (left % 2) + [4] * (left // 2)


def stage_lags(sizes):
    steps = [LAGS[0]] + [LAGS[1] if size == 2 else LAGS[2] for size in sizes[1:]]
    steps = steps + steps[::-1]
    return [sum(steps[: stage + 1]) for stage in range(len(steps))]


def box_kernel(
    sizes, lags, norm, weights_hbm, cut_x_hbm, cut_y_hbm, index_hbm, field_hbm, table_hbm, base_hbm,
    turn_hbm, host_hbm, mix_hbm, back_hbm, full_ref, edge_ref, kept_field_ref, back_ref, x_ref,
    part_ref, want_ref, scale_ref, three_ref, table_ref, base_ref, turn_ref, host_ref, mix_ref,
    weights_ref, cut_x_ref, cut_y_ref, index_ref, *scratch
):
    phases = len(sizes)
    got, kept = scratch[:phases], scratch[phases : 2 * phases - 1]
    send_sem, recv_sem, load_sem, fetch_sem = scratch[2 * phases - 1 :]
    fields, row_count, ny = kept_field_ref.shape
    chunks, span, kbox = scale_ref.shape
    group = fields // chunks
    owned, khalf, levels = span // group, kbox // 2, cut_x_ref.shape[0]
    variables = fields // levels
    half = owned // 2
    me = lax.axis_index("row")
    member = lax.axis_index("member")
    strides = [1]
    for size in sizes:
        strides.append(strides[-1] * size)
    mine = [(me // strides[s]) % sizes[s] for s in range(phases)]
    barrier = pltpu.get_barrier_semaphore()

    def digit(step, away):
        return (mine[step] + away) % sizes[step]

    def peer(step, away):
        return (member, me + (digit(step, away) - mine[step]) * strides[step])

    def others(step):
        return range(1, sizes[step])

    def load(chunk):
        block = pl.ds(chunk * group, group)
        return pltpu.make_async_copy(
            field_hbm.at[block], kept_field_ref.at[block], load_sem.at[chunk]
        )

    early = [(table_hbm, table_ref), (base_hbm, base_ref), (turn_hbm.at[me], turn_ref)]
    late = [
        (host_hbm, host_ref), (mix_hbm, mix_ref), (weights_hbm, weights_ref),
        (cut_x_hbm, cut_x_ref), (cut_y_hbm, cut_y_ref), (index_hbm, index_ref),
    ]
    last = [(back_hbm, back_ref)]
    fetches = [
        pltpu.make_async_copy(source, target, fetch_sem.at[place])
        for place, (source, target) in enumerate(early + late + last)
    ]
    early, late, last = fetches[:3], fetches[3:9], fetches[9:]

    load(0).start()
    for fetch in early:
        fetch.start()
    for fetch in late:
        fetch.start()
    for chunk in range(1, min(AHEAD, chunks)):
        load(chunk).start()
    for step in range(phases):
        for away in others(step):
            pl.semaphore_signal(barrier, inc=1, device_id=peer(step, away), device_id_type=MESH)

    def lead(step, value):
        return (slice(None),) * (phases - 1 - step) + (value,)

    def remote(source, target, stage, chunk, step, away):
        return pltpu.make_async_remote_copy(
            src_ref=source,
            dst_ref=target,
            send_sem=send_sem.at[chunk, stage, away - 1],
            recv_sem=recv_sem.at[chunk, stage, away - 1],
            device_id=peer(step, away),
            device_id_type=MESH,
        )

    def held(step):
        return part_ref if step == 0 else kept[step - 1]

    def reduce_copy(step, chunk, away):
        source = held(step).at[(chunk,) + lead(step, digit(step, away))]
        return remote(source, got[step].at[chunk, away - 1], step, chunk, step, away)

    def gather_copy(step, chunk, away):
        fixed = tuple(mine[s] for s in range(step, -1, -1))
        block = full_ref.at[(chunk,) + (slice(None),) * (phases - 1 - step) + fixed]
        return remote(block, block, 2 * phases - 1 - step, chunk, step, away)

    def mixed(values):
        total = 0.0
        for _ in range(3):
            piece = values.astype(jnp.bfloat16)
            values = values - piece.astype(jnp.float32)
            total = total + lax.dot_general(
                piece,
                mix_ref[...],
                (((1,), (1,)), ((), ())),
                preferred_element_type=jnp.float32,
            )
        return total

    def prepare():
        for fetch in late:
            fetch.wait()
        edge = cut_x_ref[0]
        for level in range(levels):
            edge = jnp.maximum(edge, jnp.maximum(cut_x_ref[level], cut_y_ref[level]))
        edge_ref[0] = edge
        cosine, sine = [], []
        for place in range(owned):
            pair = 2 * (place % (half // 2)) + place // half
            plus, minus = host_ref[2 * pair], host_ref[2 * pair + 1]
            if pair == 0:
                minus = jnp.where(me == 0, 0.0, minus)
            if place // (half // 2) % 2 == 0:
                cosine.append(plus[0] + minus[0])
                sine.append(-(plus[1] + minus[1]))
            else:
                cosine.append(minus[1] - plus[1])
                sine.append(minus[0] - plus[0])
        rows = owned * fields
        cosine = jnp.stack(cosine).reshape(rows, kbox)
        sine = jnp.stack(sine).reshape(rows, kbox)
        modes = mixed(jnp.concatenate([cosine, sine], 1))
        slot = lax.broadcasted_iota(jnp.int32, (owned, kbox), 0)
        wave = me * half + 2 * (slot % (half // 2)) + slot // half
        across = lax.broadcasted_iota(jnp.int32, (owned, kbox), 1) % khalf
        times = jnp.where(wave == 0, 1.0, 2.0) * jnp.where(across == 0, norm, 2.0 * norm)
        for field in range(fields):
            variable, level = divmod(field, levels)
            chunk, place = divmod(field, group)
            inside = (across <= cut_x_ref[level]) & (wave <= cut_y_ref[level])
            scale = jnp.where(inside, weights_ref[variable, index_ref[level]], 0.0)
            wanted = [
                modes[(s * levels + level) * variables + variable][None] for s in range(owned)
            ]
            block = pl.ds(place * owned, owned)
            want_ref[chunk, block] = scale * jnp.concatenate(wanted, 0)
            scale_ref[chunk, block] = scale * times

    def advance(stage, chunk):
        if stage < phases:
            total = held(stage)[(chunk,) + lead(stage, mine[stage])]
            for away in others(stage):
                reduce_copy(stage, chunk, away).wait()
                total = total + got[stage][chunk, away - 1]
            if stage + 1 < phases:
                kept[stage][chunk] = total
                for away in others(stage + 1):
                    reduce_copy(stage + 1, chunk, away).start()
            else:
                own = tuple(mine[s] for s in range(phases - 1, -1, -1))
                full_ref[(chunk,) + own] = want_ref[chunk] - scale_ref[chunk] * total
                for away in others(phases - 1):
                    gather_copy(phases - 1, chunk, away).start()
        else:
            step = 2 * phases - 1 - stage
            for away in others(step):
                gather_copy(step, chunk, away).wait()
            if step > 0:
                for away in others(step - 1):
                    gather_copy(step - 1, chunk, away).start()

    def transform(chunk):
        load(chunk).wait()

        @pl.when(chunk + AHEAD < chunks)
        def _():
            load(chunk + AHEAD).start()

        block = kept_field_ref[pl.ds(chunk * group, group)].reshape(group * row_count, ny)
        high, low = halves(block)
        both = jnp.dot(high, table_ref[...], preferred_element_type=jnp.float32)
        rest = jnp.dot(low, table_ref[:, :kbox], preferred_element_type=jnp.float32)
        part = both[:, :kbox] + both[:, kbox:] + rest
        cube = tuple(reversed(sizes))
        for k in range(group):
            high, low = halves(part[k * row_count : (k + 1) * row_count])
            moded = lax.dot_general(
                jnp.concatenate([high, low, high], 0),
                three_ref[...],
                (((0,), (0,)), ((), ())),
                preferred_element_type=jnp.float32,
            )
            where = (chunk,) + (slice(None),) * phases + (slice(k * owned, (k + 1) * owned),)
            part_ref[where] = moded.reshape(cube + (owned, kbox))

    for fetch in early:
        fetch.wait()
    turns = turn_ref[...]
    local = base_ref[:row_count] * turns[:1] + base_ref[row_count:] * turns[1:]
    x_high, x_low = halves(local)
    three_ref[...] = jnp.concatenate([x_high, x_high, x_low], 0)
    x_ref[...] = jnp.concatenate([x_high, x_high, x_low], 1)

    def tick(now, _):
        @pl.when(now < chunks)
        def _():
            transform(now)

        @pl.when(now == 0)
        def _():
            pl.semaphore_wait(barrier, sum(size - 1 for size in sizes))

        @pl.when(now < chunks)
        def _():
            for away in others(0):
                reduce_copy(0, now, away).start()

        @pl.when(now == PREPARE)
        def _():
            prepare()

        @pl.when(now == chunks - 1)
        def _():
            for fetch in last:
                fetch.start()

        for stage in range(2 * phases):
            chunk = now - lags[stage]

            @pl.when((chunk >= 0) & (chunk < chunks))
            def _(stage=stage, chunk=chunk):
                advance(stage, chunk)

        for chunk in range(READY):

            @pl.when(now == lags[-1] + 1 + chunk)
            def _(chunk=chunk):
                if chunk == 0:
                    for fetch in last:
                        fetch.wait()
                block = kept_field_ref.at[pl.ds(chunk * group, group)]
                modes = full_ref[chunk].reshape(math.prod(sizes), span, kbox)
                inverse_step(group, block, modes, back_ref, x_ref, block)

        return 0

    lax.fori_loop(0, chunks + lags[-1], tick, 0)


def box_modes(devices, chunks, scalars, field, table, base, turn, host, mix, back):
    fields, row_count, ny = field.shape
    owned, kbox = host.shape[0], host.shape[-1]
    span = fields // chunks * owned
    sizes = radices(devices)
    phases = len(sizes)
    cube = tuple(reversed(sizes))
    lags = stage_lags(sizes)

    def buffer(*shape):
        return pltpu.VMEM(shape + (span, kbox), jnp.float32)

    def like(array):
        return pltpu.VMEM(array.shape, array.dtype)

    got = [buffer(chunks, sizes[s] - 1, *cube[: phases - 1 - s]) for s in range(phases)]
    kept = [buffer(chunks, *cube[: phases - 1 - s]) for s in range(phases - 1)]
    smem = pl.BlockSpec(memory_space=pltpu.SMEM)
    vmem = pl.BlockSpec(memory_space=pltpu.VMEM)
    anywhere = pl.BlockSpec(memory_space=pl.ANY)
    widest = max(sizes) - 1
    return pl.pallas_call(
        functools.partial(box_kernel, sizes, lags, 1.0 / (row_count * devices * ny)),
        out_shape=(
            buffer(chunks, *cube),
            jax.ShapeDtypeStruct((1,), jnp.int32),
            pltpu.VMEM(field.shape, jnp.float32),
            like(back),
            pltpu.VMEM((row_count, 3 * kbox), jnp.bfloat16),
        ),
        in_specs=[anywhere] * 11,
        out_specs=(vmem, smem, vmem, vmem, vmem),
        scratch_shapes=[buffer(chunks, *cube)]
        + [buffer(chunks)] * 2
        + [pltpu.VMEM((3 * row_count, kbox), jnp.bfloat16)]
        + [like(table), like(base), pltpu.VMEM(turn.shape[1:], turn.dtype), like(host), like(mix)]
        + [pltpu.SMEM(array.shape, array.dtype) for array in scalars]
        + got
        + kept
        + [
            pltpu.SemaphoreType.DMA((chunks, 2 * phases, widest)),
            pltpu.SemaphoreType.DMA((chunks, 2 * phases, widest)),
            pltpu.SemaphoreType.DMA((chunks,)),
            pltpu.SemaphoreType.DMA((10,)),
        ],
        compiler_params=pltpu.CompilerParams(
            collective_id=0, has_side_effects=True, vmem_limit_bytes=VMEM_BYTES
        ),
    )(*scalars, field, table, base, turn, host, mix, back)


def nudge(field, host, weights, cut_x, cut_y, table_index):
    variables, levels, row_count, ny = field.shape
    owned, kbox = host.shape[0], host.shape[-1]
    khalf, half = kbox // 2, owned // 2
    devices = lax.axis_size("row")
    nx = row_count * devices
    fields = variables * levels
    group = max(size for size in range(1, GROUP + 1) if fields % size == 0)
    chunks = fields // group

    column = np.arange(kbox)
    y_odd, y_sine, y_place = column // half % 2, column // (half // 2) % 2 == 1, column % (half // 2)
    y_wave = column // owned * half + 2 * y_place + y_odd
    y_high, y_low = np_halves(real_modes(ny, ny, y_wave, y_sine))
    table_y = jnp.asarray(np.concatenate([y_high, y_low], 1))
    backs = []
    for odd in (0, 1):
        twin = np.where(y_odd == odd, column, (column + half) % owned + column // owned * owned)
        high, low = np_halves(real_modes(ny // 2, ny, y_wave[twin], y_sine[twin]).T)
        backs.append(np.concatenate([high, low], 0))
    table_back = jnp.asarray(np.stack(backs))
    x_wave, x_sine = column % khalf, column >= khalf
    start = np.arange(devices) * row_count
    base = np.concatenate(
        [real_modes(row_count, nx, x_wave, column < 0), real_modes(row_count, nx, x_wave, column >= 0)]
    )
    turn_cos = real_modes(start, nx, x_wave, column < 0)
    turn_sin = real_modes(start, nx, x_wave, column >= 0)
    turn = np.stack(
        [np.where(x_sine, turn_sin, turn_cos), np.where(x_sine, turn_cos, -turn_sin)], 1
    )
    base = jnp.asarray(base.astype(np.float32))
    turn = jnp.asarray(turn.astype(np.float32))
    wave = column - khalf
    inside = np.abs(wave) < khalf
    mc = ((column[:, None] == np.abs(wave)[None, :]) & inside).astype(np.float32)
    ms = ((column[:, None] == np.abs(wave)[None, :] + khalf) & inside) * np.sign(wave)
    ms = ms.astype(np.float32)

    span = group * owned
    modes, edge, kept_field, back, local = box_modes(
        devices,
        chunks,
        (weights.T, cut_x, cut_y, table_index),
        field.reshape(fields, row_count, ny),
        table_y,
        base,
        turn,
        host.transpose(0, 1, 3, 2, 4),
        jnp.asarray(np.concatenate([mc, ms], 1)).astype(jnp.bfloat16),
        table_back,
    )
    modes = modes.reshape(chunks, devices, span, kbox)

    def inverse(kept_field, modes, back, local):
        split = (chunks, group, row_count, ny)
        vmem = pl.BlockSpec(memory_space=pltpu.VMEM)
        result = pl.pallas_call(
            inverse_kernel,
            out_shape=jax.ShapeDtypeStruct(split, jnp.float32),
            in_specs=[vmem] * 4,
            out_specs=pl.BlockSpec(memory_space=pl.ANY),
            scratch_shapes=[
                pltpu.VMEM(split, jnp.float32), pltpu.SemaphoreType.DMA((chunks,))
            ],
            compiler_params=pltpu.CompilerParams(vmem_limit_bytes=VMEM_BYTES),
        )(kept_field.reshape(split), modes, back, local)
        return result.reshape(field.shape)

    return lax.cond(
        edge[0] >= khalf,
        lambda *args: general(*args[:6]),
        lambda *args: inverse(*args[6:]),
        field, host, weights, cut_x, cut_y, table_index, kept_field, modes, back, local,
    )


def solution(mesh):
    return jax.shard_map(
        nudge,
        mesh=mesh,
        in_specs=(
            P("member", None, "row", None),
            P("row", None, "member", None, None),
            P(),
            P(),
            P(),
            P(),
        ),
        out_specs=P("member", None, "row", None),
        check_vma=False,
    )
```

```python
import functools
import math

import jax
import jax.numpy as jnp
import numpy as np
from jax import lax
from jax.experimental import pallas as pl
from jax.experimental.pallas import tpu as pltpu
from jax.sharding import PartitionSpec as P

TABLE = 8
MESH = pl.DeviceIdType.MESH
VMEM_BYTES = 36_000_000
GROUP = 3
LAGS = (1, 2, 2)
PREPARE = 3
READY = 1
AHEAD = 3
HIGHEST = lax.Precision.HIGHEST


def box_wave(index, khalf):
    half = index // 2
    return jnp.where(index % 2 == 0, half, jnp.where(index == 1, -khalf, -half))


def wave_tables(positions, length, waves):
    phase = jnp.mod(positions[:, None] * waves[None, :], length).astype(jnp.float32) * (
        2.0 * math.pi / length
    )
    return (jnp.cos(phase), jnp.sin(phase))


def general(field, host, weights, cut_x, cut_y, table_index):
    variables, levels, row_count, ny = field.shape
    owned, kbox = host.shape[0], host.shape[-1]
    fields = variables * levels
    devices = lax.axis_size("row")
    nx = row_count * devices
    place = lax.axis_index("row")
    local_rows = place * row_count + lax.iota(jnp.int32, row_count)
    x_waves = lax.iota(jnp.int32, kbox) - kbox // 2
    y_waves = box_wave(lax.iota(jnp.int32, kbox), kbox // 2)
    own_waves = box_wave(place * owned + lax.iota(jnp.int32, owned), kbox // 2)
    onehot = (table_index[:, None] == lax.iota(jnp.int32, TABLE)[None, :]).astype(jnp.float32)
    blend = jnp.dot(onehot, weights, precision=HIGHEST)
    mask_x = (jnp.abs(x_waves)[None, :] <= cut_x[:, None]).astype(jnp.float32)
    mask_y = (jnp.abs(own_waves)[None, :] <= cut_y[:, None]).astype(jnp.float32)
    scale = blend.T[:, :, None, None] * mask_y[None, :, :, None] * mask_x[None, :, None, :]
    cos_y, sin_y = wave_tables(lax.iota(jnp.int32, ny), ny, y_waves)
    cos_x, sin_x = wave_tables(local_rows, nx, x_waves)
    table_y = jnp.concatenate([cos_y, -sin_y], 1)
    table_x = jnp.stack([jnp.concatenate([cos_x, -sin_x], 1), jnp.concatenate([sin_x, cos_x], 1)])

    def one(pair):
        grid, wanted, factor = pair
        spread = jnp.dot(grid, table_y, precision=HIGHEST).reshape(row_count, 2, kbox)
        parts = jnp.einsum("xck,cxq->kq", spread, table_x, precision=HIGHEST)
        parts = parts.reshape(devices, owned, 2, kbox)
        moved = lax.all_to_all(parts, "row", split_axis=0, concat_axis=0, tiled=True)
        spectrum = jnp.sum(moved, 0) / (nx * ny)
        delta = factor[:, None, :] * (wanted - spectrum)
        box = lax.all_gather(delta, "row", axis=0, tiled=True).reshape(kbox, 2 * kbox)
        back = jnp.einsum("kq,cxq->xck", box, table_x, precision=HIGHEST)
        return grid + jnp.dot(back.reshape(row_count, 2 * kbox), table_y.T, precision=HIGHEST)

    wanted = host.transpose(2, 3, 0, 1, 4).reshape(fields, owned, 2, kbox)
    result = lax.map(
        one, (field.reshape(fields, row_count, ny), wanted, scale.reshape(fields, owned, kbox))
    )
    return result.reshape(field.shape)


def halves(values):
    high = values.astype(jnp.bfloat16)
    return high, (values - high.astype(jnp.float32)).astype(jnp.bfloat16)


def np_halves(values):
    values = values.astype(np.float32)
    high = values.astype(jnp.bfloat16)
    return high, (values - high.astype(np.float32)).astype(jnp.bfloat16)


def real_modes(positions, length, waves, is_sine):
    if isinstance(positions, int):
        positions = np.arange(positions)
    phase = (positions[:, None] * waves[None, :]) % length * (2.0 * np.pi / length)
    return np.where(is_sine[None, :], np.sin(phase), np.cos(phase))


def inverse_kernel(field_ref, modes_ref, back_ref, x_ref, out_hbm, out_ref, sem):
    chunks, count = field_ref.shape[:2]

    def store(chunk, source):
        return pltpu.make_async_copy(source.at[chunk], out_hbm.at[chunk], sem.at[chunk])

    def step(chunk, _):
        inverse_step(count, field_ref.at[chunk], modes_ref[chunk], back_ref, x_ref, out_ref.at[chunk])
        store(chunk, out_ref).start()
        return 0

    for chunk in range(READY):
        store(chunk, field_ref).start()
    lax.fori_loop(READY, chunks, step, 0)
    for chunk in range(chunks):
        store(chunk, field_ref if chunk < READY else out_ref).wait()


def inverse_step(count, field_ref, modes, back_ref, x_ref, out_ref):
    row_count, ny = field_ref.shape[1:]
    kbox = x_ref.shape[1] // 3
    owned = modes.shape[1] // count
    parts = []
    for k in range(count):
        block = modes[:, k * owned : (k + 1) * owned]
        swapped = jnp.concatenate([block[:, owned // 2 :], block[:, : owned // 2]], 1)
        both = jnp.concatenate([block.reshape(kbox, kbox), swapped.reshape(kbox, kbox)], 0)
        high, low = halves(both)
        parts.append(
            lax.dot_general(
                x_ref[...],
                jnp.concatenate([high, low, high], 1),
                (((1,), (1,)), ((), ())),
                preferred_element_type=jnp.float32,
            )
        )
    spread = jnp.concatenate(parts, 0)
    high = spread[:, :kbox].astype(jnp.bfloat16)
    low = (spread[:, kbox:] - spread[:, kbox:].astype(jnp.bfloat16).astype(jnp.float32)).astype(
        jnp.bfloat16
    )
    lane = lax.broadcasted_iota(jnp.int32, high.shape, 1)
    first = lane % owned < owned // 2
    even = jnp.where(first, high, low)
    odd = jnp.where(first, low, high)
    shape = (count, row_count, ny // 2)
    plus = jnp.dot(
        jnp.concatenate([even, even], 1), back_ref[0], preferred_element_type=jnp.float32
    ).reshape(shape)
    minus = jnp.dot(
        jnp.concatenate([odd, odd], 1), back_ref[1], preferred_element_type=jnp.float32
    ).reshape(shape)
    out_ref[:, :, : ny // 2] = field_ref[:, :, : ny // 2] + (plus + minus)
    out_ref[:, :, ny // 2 :] = field_ref[:, :, ny // 2 :] + (plus - minus)


def radices(devices):
    bits = devices.bit_length() - 1
    sizes = [2] * min(bits, 1)
    left = bits - len(sizes)
    return sizes + [2] * (left % 2) + [4] * (left // 2)


def stage_lags(sizes):
    steps = [LAGS[0]] + [LAGS[1] if size == 2 else LAGS[2] for size in sizes[1:]]
    up = [step + (size == 2 and s > 0) for s, (step, size) in enumerate(zip(steps, sizes))]
    steps = steps + up[::-1]
    return [sum(steps[: stage + 1]) for stage in range(len(steps))]


def box_kernel(
    sizes, lags, norm, weights_hbm, cut_x_hbm, cut_y_hbm, index_hbm, field_hbm, table_hbm, base_hbm,
    turn_hbm, host_hbm, mix_hbm, back_hbm, full_ref, edge_ref, kept_field_ref, back_ref, x_ref,
    part_ref, want_ref, scale_ref, three_ref, table_ref, base_ref, turn_ref, host_ref, mix_ref,
    weights_ref, cut_x_ref, cut_y_ref, index_ref, *scratch
):
    phases = len(sizes)
    got, kept = scratch[:phases], scratch[phases : 2 * phases - 1]
    send_sem, recv_sem, load_sem, fetch_sem = scratch[2 * phases - 1 :]
    fields, row_count, ny = kept_field_ref.shape
    chunks, span, kbox = scale_ref.shape
    group = fields // chunks
    owned, khalf, levels = span // group, kbox // 2, cut_x_ref.shape[0]
    variables = fields // levels
    half = owned // 2
    me = lax.axis_index("row")
    member = lax.axis_index("member")
    strides = [1]
    for size in sizes:
        strides.append(strides[-1] * size)
    mine = [(me // strides[s]) % sizes[s] for s in range(phases)]
    barrier = pltpu.get_barrier_semaphore()

    def digit(step, away):
        return (mine[step] + away) % sizes[step]

    def peer(step, away):
        return (member, me + (digit(step, away) - mine[step]) * strides[step])

    def others(step):
        return range(1, sizes[step])

    def load(chunk):
        block = pl.ds(chunk * group, group)
        return pltpu.make_async_copy(
            field_hbm.at[block], kept_field_ref.at[block], load_sem.at[chunk]
        )

    early = [(table_hbm, table_ref), (base_hbm, base_ref), (turn_hbm.at[me], turn_ref)]
    late = [
        (host_hbm, host_ref), (mix_hbm, mix_ref), (weights_hbm, weights_ref),
        (cut_x_hbm, cut_x_ref), (cut_y_hbm, cut_y_ref), (index_hbm, index_ref),
    ]
    last = [(back_hbm, back_ref)]
    fetches = [
        pltpu.make_async_copy(source, target, fetch_sem.at[place])
        for place, (source, target) in enumerate(early + late + last)
    ]
    early, late, last = fetches[:3], fetches[3:9], fetches[9:]

    load(0).start()
    for fetch in early:
        fetch.start()
    for fetch in late:
        fetch.start()
    for chunk in range(1, min(AHEAD, chunks)):
        load(chunk).start()
    for step in range(phases):
        for away in others(step):
            pl.semaphore_signal(barrier, inc=1, device_id=peer(step, away), device_id_type=MESH)

    def lead(step, value):
        return (slice(None),) * (phases - 1 - step) + (value,)

    def remote(source, target, stage, chunk, step, away):
        return pltpu.make_async_remote_copy(
            src_ref=source,
            dst_ref=target,
            send_sem=send_sem.at[chunk, stage, away - 1],
            recv_sem=recv_sem.at[chunk, stage, away - 1],
            device_id=peer(step, away),
            device_id_type=MESH,
        )

    def held(step):
        return part_ref if step == 0 else kept[step - 1]

    def reduce_copy(step, chunk, away):
        source = held(step).at[(chunk,) + lead(step, digit(step, away))]
        return remote(source, got[step].at[chunk, away - 1], step, chunk, step, away)

    def gather_copy(step, chunk, away):
        fixed = tuple(mine[s] for s in range(step, -1, -1))
        block = full_ref.at[(chunk,) + (slice(None),) * (phases - 1 - step) + fixed]
        return remote(block, block, 2 * phases - 1 - step, chunk, step, away)

    def mixed(values):
        total = 0.0
        for _ in range(3):
            piece = values.astype(jnp.bfloat16)
            values = values - piece.astype(jnp.float32)
            total = total + lax.dot_general(
                piece,
                mix_ref[...],
                (((1,), (1,)), ((), ())),
                preferred_element_type=jnp.float32,
            )
        return total

    def prepare():
        for fetch in late:
            fetch.wait()
        edge = cut_x_ref[0]
        for level in range(levels):
            edge = jnp.maximum(edge, jnp.maximum(cut_x_ref[level], cut_y_ref[level]))
        edge_ref[0] = edge
        cosine, sine = [], []
        for place in range(owned):
            pair = 2 * (place % (half // 2)) + place // half
            plus, minus = host_ref[2 * pair], host_ref[2 * pair + 1]
            if pair == 0:
                minus = jnp.where(me == 0, 0.0, minus)
            if place // (half // 2) % 2 == 0:
                cosine.append(plus[0] + minus[0])
                sine.append(-(plus[1] + minus[1]))
            else:
                cosine.append(minus[1] - plus[1])
                sine.append(minus[0] - plus[0])
        rows = owned * fields
        cosine = jnp.stack(cosine).reshape(rows, kbox)
        sine = jnp.stack(sine).reshape(rows, kbox)
        modes = mixed(jnp.concatenate([cosine, sine], 1))
        slot = lax.broadcasted_iota(jnp.int32, (owned, kbox), 0)
        wave = me * half + 2 * (slot % (half // 2)) + slot // half
        across = lax.broadcasted_iota(jnp.int32, (owned, kbox), 1) % khalf
        times = jnp.where(wave == 0, 1.0, 2.0) * jnp.where(across == 0, norm, 2.0 * norm)
        for field in range(fields):
            variable, level = divmod(field, levels)
            chunk, place = divmod(field, group)
            inside = (across <= cut_x_ref[level]) & (wave <= cut_y_ref[level])
            scale = jnp.where(inside, weights_ref[variable, index_ref[level]], 0.0)
            wanted = [
                modes[(s * levels + level) * variables + variable][None] for s in range(owned)
            ]
            block = pl.ds(place * owned, owned)
            want_ref[chunk, block] = scale * jnp.concatenate(wanted, 0)
            scale_ref[chunk, block] = scale * times

    def advance(stage, chunk):
        if stage < phases:
            total = held(stage)[(chunk,) + lead(stage, mine[stage])]
            for away in others(stage):
                reduce_copy(stage, chunk, away).wait()
                total = total + got[stage][chunk, away - 1]
            if stage + 1 < phases:
                kept[stage][chunk] = total
                for away in others(stage + 1):
                    reduce_copy(stage + 1, chunk, away).start()
            else:
                own = tuple(mine[s] for s in range(phases - 1, -1, -1))
                full_ref[(chunk,) + own] = want_ref[chunk] - scale_ref[chunk] * total
                for away in others(phases - 1):
                    gather_copy(phases - 1, chunk, away).start()
        else:
            step = 2 * phases - 1 - stage
            for away in others(step):
                gather_copy(step, chunk, away).wait()
            if step > 0:
                for away in others(step - 1):
                    gather_copy(step - 1, chunk, away).start()

    def transform(chunk):
        load(chunk).wait()

        @pl.when(chunk + AHEAD < chunks)
        def _():
            load(chunk + AHEAD).start()

        block = kept_field_ref[pl.ds(chunk * group, group)].reshape(group * row_count, ny)
        high, low = halves(block)
        both = jnp.dot(high, table_ref[...], preferred_element_type=jnp.float32)
        rest = jnp.dot(low, table_ref[:, :kbox], preferred_element_type=jnp.float32)
        part = both[:, :kbox] + both[:, kbox:] + rest
        cube = tuple(reversed(sizes))
        for k in range(group):
            high, low = halves(part[k * row_count : (k + 1) * row_count])
            moded = lax.dot_general(
                jnp.concatenate([high, low, high], 0),
                three_ref[...],
                (((0,), (0,)), ((), ())),
                preferred_element_type=jnp.float32,
            )
            where = (chunk,) + (slice(None),) * phases + (slice(k * owned, (k + 1) * owned),)
            part_ref[where] = moded.reshape(cube + (owned, kbox))

    for fetch in early:
        fetch.wait()
    turns = turn_ref[...]
    local = base_ref[:row_count] * turns[:1] + base_ref[row_count:] * turns[1:]
    x_high, x_low = halves(local)
    three_ref[...] = jnp.concatenate([x_high, x_high, x_low], 0)
    x_ref[...] = jnp.concatenate([x_high, x_high, x_low], 1)

    def tick(now, _):
        @pl.when(now < chunks)
        def _():
            transform(now)

        @pl.when(now == 0)
        def _():
            pl.semaphore_wait(barrier, sum(size - 1 for size in sizes))

        @pl.when(now < chunks)
        def _():
            for away in others(0):
                reduce_copy(0, now, away).start()

        @pl.when(now == PREPARE)
        def _():
            prepare()

        @pl.when(now == chunks - 1)
        def _():
            for fetch in last:
                fetch.start()

        for stage in range(2 * phases):
            chunk = now - lags[stage]

            @pl.when((chunk >= 0) & (chunk < chunks))
            def _(stage=stage, chunk=chunk):
                advance(stage, chunk)

        for chunk in range(READY):

            @pl.when(now == lags[-1] + 1 + chunk)
            def _(chunk=chunk):
                if chunk == 0:
                    for fetch in last:
                        fetch.wait()
                block = kept_field_ref.at[pl.ds(chunk * group, group)]
                modes = full_ref[chunk].reshape(math.prod(sizes), span, kbox)
                inverse_step(group, block, modes, back_ref, x_ref, block)

        return 0

    lax.fori_loop(0, chunks + lags[-1], tick, 0)


def box_modes(devices, chunks, scalars, field, table, base, turn, host, mix, back):
    fields, row_count, ny = field.shape
    owned, kbox = host.shape[0], host.shape[-1]
    span = fields // chunks * owned
    sizes = radices(devices)
    phases = len(sizes)
    cube = tuple(reversed(sizes))
    lags = stage_lags(sizes)

    def buffer(*shape):
        return pltpu.VMEM(shape + (span, kbox), jnp.float32)

    def like(array):
        return pltpu.VMEM(array.shape, array.dtype)

    got = [buffer(chunks, sizes[s] - 1, *cube[: phases - 1 - s]) for s in range(phases)]
    kept = [buffer(chunks, *cube[: phases - 1 - s]) for s in range(phases - 1)]
    smem = pl.BlockSpec(memory_space=pltpu.SMEM)
    vmem = pl.BlockSpec(memory_space=pltpu.VMEM)
    anywhere = pl.BlockSpec(memory_space=pl.ANY)
    widest = max(sizes) - 1
    return pl.pallas_call(
        functools.partial(box_kernel, sizes, lags, 1.0 / (row_count * devices * ny)),
        out_shape=(
            buffer(chunks, *cube),
            jax.ShapeDtypeStruct((1,), jnp.int32),
            pltpu.VMEM(field.shape, jnp.float32),
            like(back),
            pltpu.VMEM((row_count, 3 * kbox), jnp.bfloat16),
        ),
        in_specs=[anywhere] * 11,
        out_specs=(vmem, smem, vmem, vmem, vmem),
        scratch_shapes=[buffer(chunks, *cube)]
        + [buffer(chunks)] * 2
        + [pltpu.VMEM((3 * row_count, kbox), jnp.bfloat16)]
        + [like(table), like(base), pltpu.VMEM(turn.shape[1:], turn.dtype), like(host), like(mix)]
        + [pltpu.SMEM(array.shape, array.dtype) for array in scalars]
        + got
        + kept
        + [
            pltpu.SemaphoreType.DMA((chunks, 2 * phases, widest)),
            pltpu.SemaphoreType.DMA((chunks, 2 * phases, widest)),
            pltpu.SemaphoreType.DMA((chunks,)),
            pltpu.SemaphoreType.DMA((10,)),
        ],
        compiler_params=pltpu.CompilerParams(
            collective_id=0, has_side_effects=True, vmem_limit_bytes=VMEM_BYTES
        ),
    )(*scalars, field, table, base, turn, host, mix, back)


def nudge(field, host, weights, cut_x, cut_y, table_index):
    variables, levels, row_count, ny = field.shape
    owned, kbox = host.shape[0], host.shape[-1]
    khalf, half = kbox // 2, owned // 2
    devices = lax.axis_size("row")
    nx = row_count * devices
    fields = variables * levels
    group = max(size for size in range(1, GROUP + 1) if fields % size == 0)
    chunks = fields // group

    column = np.arange(kbox)
    y_odd, y_sine, y_place = column // half % 2, column // (half // 2) % 2 == 1, column % (half // 2)
    y_wave = column // owned * half + 2 * y_place + y_odd
    y_high, y_low = np_halves(real_modes(ny, ny, y_wave, y_sine))
    table_y = jnp.asarray(np.concatenate([y_high, y_low], 1))
    backs = []
    for odd in (0, 1):
        twin = np.where(y_odd == odd, column, (column + half) % owned + column // owned * owned)
        high, low = np_halves(real_modes(ny // 2, ny, y_wave[twin], y_sine[twin]).T)
        backs.append(np.concatenate([high, low], 0))
    table_back = jnp.asarray(np.stack(backs))
    x_wave, x_sine = column % khalf, column >= khalf
    start = np.arange(devices) * row_count
    base = np.concatenate(
        [real_modes(row_count, nx, x_wave, column < 0), real_modes(row_count, nx, x_wave, column >= 0)]
    )
    turn_cos = real_modes(start, nx, x_wave, column < 0)
    turn_sin = real_modes(start, nx, x_wave, column >= 0)
    turn = np.stack(
        [np.where(x_sine, turn_sin, turn_cos), np.where(x_sine, turn_cos, -turn_sin)], 1
    )
    base = jnp.asarray(base.astype(np.float32))
    turn = jnp.asarray(turn.astype(np.float32))
    wave = column - khalf
    inside = np.abs(wave) < khalf
    mc = ((column[:, None] == np.abs(wave)[None, :]) & inside).astype(np.float32)
    ms = ((column[:, None] == np.abs(wave)[None, :] + khalf) & inside) * np.sign(wave)
    ms = ms.astype(np.float32)

    span = group * owned
    modes, edge, kept_field, back, local = box_modes(
        devices,
        chunks,
        (weights.T, cut_x, cut_y, table_index),
        field.reshape(fields, row_count, ny),
        table_y,
        base,
        turn,
        host.transpose(0, 1, 3, 2, 4),
        jnp.asarray(np.concatenate([mc, ms], 1)).astype(jnp.bfloat16),
        table_back,
    )
    modes = modes.reshape(chunks, devices, span, kbox)

    def inverse(kept_field, modes, back, local):
        split = (chunks, group, row_count, ny)
        vmem = pl.BlockSpec(memory_space=pltpu.VMEM)
        result = pl.pallas_call(
            inverse_kernel,
            out_shape=jax.ShapeDtypeStruct(split, jnp.float32),
            in_specs=[vmem] * 4,
            out_specs=pl.BlockSpec(memory_space=pl.ANY),
            scratch_shapes=[
                pltpu.VMEM(split, jnp.float32), pltpu.SemaphoreType.DMA((chunks,))
            ],
            compiler_params=pltpu.CompilerParams(vmem_limit_bytes=VMEM_BYTES),
        )(kept_field.reshape(split), modes, back, local)
        return result.reshape(field.shape)

    return lax.cond(
        edge[0] >= khalf,
        lambda *args: general(*args[:6]),
        lambda *args: inverse(*args[6:]),
        field, host, weights, cut_x, cut_y, table_index, kept_field, modes, back, local,
    )


def solution(mesh):
    return jax.shard_map(
        nudge,
        mesh=mesh,
        in_specs=(
            P("member", None, "row", None),
            P("row", None, "member", None, None),
            P(),
            P(),
            P(),
            P(),
        ),
        out_specs=P("member", None, "row", None),
        check_vma=False,
    )
```
